32 devices in a mesh: bl: 8 (over z, x), tm: 4 (over y, core).
Axes of the slice: x: 2, y: 2, z: 4, core: 2. Of those that a mesh axis runs over, the one named last changes fastest.
Arguments:
- visibility_real: bfloat16 [3072, 16, 1024], P('bl', 'tm'), may hold values from -6 to 6
- visibility_imag: bfloat16 [3072, 16, 1024], P('bl', 'tm'), may hold values from -6 to 6
- weights: int32 [3072, 16], P('bl', 'tm'), may hold values from 0 to 8
- labels: int32 [3072], P('bl'), may hold values from 0 to 511, as said below
- owner_of: int32 [512], replicated, may hold values from 0 to 7, as said below
Outputs:
- bandpower: float32 [512, 1024], P(('bl', 'tm'))
The draws below stay inside these ranges and needn't reach their ends.
Inputs may be any that keep to these rules, and one draw needn't show every extreme that they name: Of the rows of one device, at most 72 have labels of groups with one owner, and these carry at most 18 different labels; in every draw some owner gets exactly 72 such rows with exactly 18 labels from every device. `owner_of`: every owner owns exactly 64 groups.
All inputs are finite; a program needn't handle non-finite values.
Results may differ from the reference program's by a relative error of at most 0.0003.
Values may be sent and summed in bfloat16 or wider, within the bound.
No kernel may reach another device: no remote copies, remote signals or barrier semaphores. Data moves between devices by JAX's collectives and lax.ppermute only.
A program may use at most 128 MiB of HBM per device.

```python
import math
import jax
import jax.numpy as jnp
from jax import lax

FREQ_CHANNELS = 1024
B_DEV = 384
G_DEV = 64
BASELINE_COUNT = 3072
TIME_STEPS = 16
CAP = 72
KEYS = 18
N_BL = 8


def layout_plan(key):
    groups = G_DEV * N_BL
    group_order = jax.random.permutation(jax.random.fold_in(key, 101), groups).astype(jnp.int32)
    owner_of = jnp.zeros((groups,), jnp.int32).at[group_order].set(jnp.arange(groups, dtype=jnp.int32) // G_DEV)
    heaviest_owner = jax.random.randint(jax.random.fold_in(key, 102), (), 0, N_BL)

    def one_device(device):
        device_key = jax.random.fold_in(jax.random.fold_in(key, 103), device)
        slot_ids = jnp.arange(N_BL * CAP, dtype=jnp.int32)
        priority = jax.random.permutation(jax.random.fold_in(device_key, 1), N_BL * CAP).astype(jnp.int32)
        priority = jnp.where(slot_ids // CAP == heaviest_owner, priority - N_BL * CAP, priority)
        chosen = jnp.argsort(priority)[:B_DEV].astype(jnp.int32)
        target = chosen // CAP
        within = chosen % CAP

        def candidates(owner):
            owner_key = jax.random.fold_in(jax.random.fold_in(device_key, 2), owner)
            return jax.random.permutation(owner_key, G_DEV)[:KEYS].astype(jnp.int32)
        offsets = jax.vmap(candidates)(jnp.arange(N_BL, dtype=jnp.int32))
        picked = offsets[target, within % KEYS]
        row_label = group_order[target * G_DEV + picked]
        shuffle = jax.random.permutation(jax.random.fold_in(device_key, 3), B_DEV)
        return row_label[shuffle]
    labels = jax.vmap(one_device)(jnp.arange(N_BL, dtype=jnp.int32)).reshape(-1)
    return (labels.astype(jnp.int32), owner_of)


def draw_labels(key, part):
    return layout_plan(key)[0]


def draw_owner_of(key, part):
    return layout_plan(key)[1]


def set_ends(values, stream_key, low, top_value):
    dims = values.shape
    index_at = [jax.random.randint(jax.random.fold_in(stream_key, axis), (), 0, dims[axis]) for axis in range(len(dims))]
    values = values.at[tuple(index_at)].set(low)
    longest = dims.index(max(dims))
    index_at[longest] = (index_at[longest] + 1) % dims[longest]
    return values.at[tuple(index_at)].set(top_value)


def shard_levels(key, dims, split, smallest, largest):
    loudness = 1.0
    for dim, blocks in split:
        draws = jax.random.uniform(jax.random.fold_in(jax.random.fold_in(key, 6), dim), (blocks,), jnp.float32, smallest / len(split), largest / len(split))
        loudness = loudness * jnp.repeat(jnp.exp(draws), dims[dim] // blocks).reshape((-1,) + (1,) * (len(dims) - 1 - dim))
    return loudness


def noise(key, shape, width, reach, shards=(), kind=jnp.bfloat16):
    level = shard_levels(key, shape, shards, -0.22, 0.18) if shards else 1.0
    array = jax.random.normal(key, shape, jnp.float32) * width * level
    return jnp.minimum(jnp.maximum(array, -reach), reach).astype(kind)


def setup_inputs(seed: int = 0) -> dict:
    keys = jax.random.split(jax.random.key(seed), 6)
    return {
        "visibility_real": noise(keys[0], (BASELINE_COUNT, TIME_STEPS, FREQ_CHANNELS), 1.0, 6.0, ((0, 8), (1, 4))),
        "visibility_imag": noise(keys[1], (BASELINE_COUNT, TIME_STEPS, FREQ_CHANNELS), 1.0, 6.0, ((0, 8), (1, 4))),
        "weights": set_ends(jax.random.randint(keys[2], (BASELINE_COUNT, TIME_STEPS), 0, 9), jax.random.fold_in(keys[2], 1), 0, 8).astype(jnp.int32),
        "labels": draw_labels(jax.random.fold_in(keys[5], 71), 0),
        "owner_of": draw_owner_of(jax.random.fold_in(keys[5], 71), 0),
    }


HARRIS = (0.35875, 0.48829, 0.14128, 0.01168)

def taper_of(length):
    phase_angle = 2.0 * math.pi / length * jnp.arange(length, dtype=jnp.float32)
    return HARRIS[0] - HARRIS[1] * jnp.cos(phase_angle) + HARRIS[2] * jnp.cos(2.0 * phase_angle) - HARRIS[3] * jnp.cos(3.0 * phase_angle)

def reference(visibility_real, visibility_imag, weights, labels, owner_of):
    groups = owner_of.shape[0]
    channels = visibility_real.shape[2]
    times = visibility_real.shape[1]
    window_taper = taper_of(channels)
    window_taper = window_taper / jnp.sqrt(jnp.sum(window_taper * window_taper))

    def advance(carried, instant):
        prior_real, prior_imag, running = carried
        row_weight = lax.dynamic_index_in_dim(weights, instant, 1, keepdims=False).astype(jnp.float32)
        slab_real = lax.dynamic_index_in_dim(visibility_real, instant, 1, keepdims=False).astype(jnp.float32)
        slab_imag = lax.dynamic_index_in_dim(visibility_imag, instant, 1, keepdims=False).astype(jnp.float32)
        sum_real = jax.ops.segment_sum(row_weight[:, None] * slab_real, labels, num_segments=groups)
        sum_imag = jax.ops.segment_sum(row_weight[:, None] * slab_imag, labels, num_segments=groups)
        weight_sum = jax.ops.segment_sum(row_weight, labels, num_segments=groups)
        divisor = jnp.maximum(weight_sum, 1.0)[:, None]
        mean_real = sum_real / divisor
        mean_imag = sum_imag / divisor
        spectrum = jnp.fft.fft((mean_real + 1j * mean_imag) * window_taper[None, :], axis=1)
        spec_real = jnp.real(spectrum)
        spec_imag = jnp.imag(spectrum)
        cross = prior_real * spec_real + prior_imag * spec_imag
        running = running + jnp.where(instant > 0, cross, jnp.zeros_like(cross))
        return ((spec_real, spec_imag, running), instant)
    zeros = jnp.zeros((groups, channels), jnp.float32)
    final_state, unused = lax.scan(advance, (zeros, zeros, zeros), jnp.arange(times, dtype=jnp.int32))
    order = jnp.argsort(owner_of * groups + jnp.arange(groups, dtype=jnp.int32))
    return final_state[2][order]
```

```python
import functools
import math

import jax
import jax.numpy as jnp
import numpy as np
from jax import lax
from jax.experimental import pallas as pl
from jax.experimental.pallas import tpu as pltpu
from jax.sharding import PartitionSpec as P


HARRIS = (0.35875, 0.48829, 0.14128, 0.01168)
LANES = 128
SUBLANES = 8
RADIX = 4
HALF = 32768.0
EXP_BIAS = 80
BF16 = jnp.bfloat16
F32 = jnp.float32
I32 = jnp.int32


def up_to(value, multiple):
    return -(-value // multiple) * multiple


class Sizes:
    def __init__(self, rows, times, channels, groups, owners, parts):
        self.rows, self.times, self.channels = rows, times, channels
        self.groups, self.owners, self.parts = groups, owners, parts
        self.per_owner = groups // owners
        capacity = 3 * rows // (2 * owners)
        self.distinct = min(capacity // 4, self.per_owner // 2)
        self.stride = up_to(self.distinct, SUBLANES)
        self.slots = owners * self.stride
        self.slot_lanes = up_to(self.slots, LANES)
        self.meta_parts = self.slot_lanes // LANES
        self.meta_rows = up_to(3 * self.meta_parts, SUBLANES)
        self.tiles = channels // LANES
        self.data_rows = self.distinct * self.tiles
        self.block_rows = self.data_rows + self.meta_rows
        self.fold = rows * times
        self.short = channels // RADIX
        self.share = self.per_owner // parts


def taper_table(channels):
    angle = 2.0 * math.pi / channels * np.arange(channels, dtype=np.float64)
    window = (
        HARRIS[0]
        - HARRIS[1] * np.cos(angle)
        + HARRIS[2] * np.cos(2.0 * angle)
        - HARRIS[3] * np.cos(3.0 * angle)
    )
    window = window / np.sqrt(np.sum(window * window))
    return window.astype(np.float32)[None, :]


def short_tables(short):
    index = np.arange(short)
    angle = 2.0 * math.pi / short * (index[:, None] * index[None, :] % short)
    cosine, sine = np.cos(angle), np.sin(angle)
    table = np.block([[cosine, -sine], [sine, cosine]]).astype(np.float32)
    high = table.astype(BF16)
    low = (table - high.astype(np.float32)).astype(BF16)
    return high, low


def twiddle_table(channels):
    short = channels // RADIX
    angle = 2.0 * math.pi / channels * (np.arange(RADIX)[:, None] * np.arange(short)[None, :])
    return np.concatenate([np.cos(angle), np.sin(angle)], axis=0).astype(np.float32)


def iota(shape, dimension):
    return lax.broadcasted_iota(I32, shape, dimension)


def dot(a, b):
    return jnp.dot(a, b, preferred_element_type=F32)


def dot_rows(a, b):
    return lax.dot_general(a, b, (((1,), (1,)), ((), ())), preferred_element_type=F32)


def flag(condition):
    return jnp.where(condition, 1.0, 0.0).astype(F32)


def place_groups(z, me, labels_ref, spread_ref, owner_ref):
    distance = owner_ref[...] ^ me
    hits = flag(iota((z.owners, z.groups), 0) == distance)
    match = flag(iota((z.groups, z.rows), 0) == labels_ref[...]).astype(BF16)
    counts = dot_rows(jnp.ones((SUBLANES, z.rows), BF16), match)
    present = flag(counts[:1] > 0.5)
    before = flag(iota((z.groups, z.groups), 0) < iota((z.groups, z.groups), 1)).astype(BF16)
    stacked = jnp.concatenate([hits, hits * present], axis=0).astype(BF16)
    prefix = dot(stacked, before)
    rank = jnp.sum(hits * prefix[: z.owners], axis=0, keepdims=True)
    order = jnp.sum(hits * prefix[z.owners :], axis=0, keepdims=True)
    slot = distance.astype(F32) * z.stride + order
    spread = flag(iota((z.groups, z.fold), 0) == spread_ref[...]).astype(BF16)
    wide = jnp.broadcast_to(slot, (SUBLANES, z.groups)).astype(BF16)
    row_slot = dot(wide, spread).astype(I32)
    slot_hit = flag(
        (iota((z.slot_lanes, z.groups), 0) == slot.astype(I32)) & (present > 0.5)
    ).astype(BF16)
    ranks = jnp.broadcast_to(rank, (SUBLANES, z.groups)).astype(BF16)
    slot_rank = dot_rows(ranks, slot_hit).astype(I32)
    return row_slot, slot_rank


def fold_and_code(z, instant, row_slot, slot_rank, weight_ref, taper_ref, real, imag, outs):
    lane = iota((1, z.fold), 1)
    weight = jnp.where(lane % z.times == instant, weight_ref[...], 0).astype(F32)
    folder = jnp.where(iota((z.slots, z.fold), 0) == row_slot[:1], weight, 0.0).astype(BF16)
    taper = taper_ref[...]
    sum_real = dot(folder, real) * taper
    sum_imag = dot(folder, imag) * taper
    padded = folder
    if z.slot_lanes > z.slots:
        padded = jnp.concatenate(
            [folder, jnp.zeros((z.slot_lanes - z.slots, z.fold), BF16)], axis=0
        )
    weight_row = dot_rows(jnp.ones((SUBLANES, z.fold), BF16), padded).astype(I32)
    top = jnp.max(jnp.maximum(jnp.abs(sum_real), jnp.abs(sum_imag)), axis=1, keepdims=True)
    mantissa = jnp.maximum(top, 2.0**-EXP_BIAS) * 2.0**EXP_BIAS
    exponent = jnp.zeros_like(top)
    shrink = jnp.ones_like(top)
    for step in (64, 32, 16, 8, 4, 2, 1):
        large = mantissa >= 2.0**step
        mantissa = jnp.where(large, mantissa * 2.0**-step, mantissa)
        exponent = jnp.where(large, exponent + step, exponent)
        shrink = jnp.where(large, shrink * 2.0**-step, shrink)
    digits = jnp.ceil(mantissa * 128.0)
    inverse = (shrink * 2.0**EXP_BIAS) * (2.0**22 / digits)
    code = exponent * 512.0 + digits
    diagonal = iota((z.slots, z.slot_lanes), 0) == iota((z.slots, z.slot_lanes), 1)
    code_row = jnp.sum(jnp.where(diagonal, code, 0.0), axis=0, keepdims=True).astype(I32)
    top_code = 2.0 * HALF - 1.0
    word_real = jnp.minimum(sum_real * inverse + (HALF + 0.5), top_code).astype(I32)
    word_imag = jnp.minimum(sum_imag * inverse + (HALF + 0.5), top_code).astype(I32)
    word = (word_real << 16) | word_imag
    lines = []
    for row in (slot_rank, weight_row, code_row):
        for part in range(z.meta_parts):
            lines.append(row[:1, part * LANES : (part + 1) * LANES])
    spare = z.meta_rows - len(lines)
    if spare:
        lines.append(jnp.zeros((spare, LANES), I32))
    meta = jnp.concatenate(lines, axis=0)
    place = iota(meta.shape, 0) % z.meta_parts * LANES + iota(meta.shape, 1)
    for distance in range(z.owners):
        out = outs[distance]
        first = distance * z.stride
        for tile in range(z.tiles):
            piece = word[first : first + z.distinct, tile * LANES : (tile + 1) * LANES]
            out[pl.ds(tile, z.distinct, stride=z.tiles), :] = piece
        mine = (place >= first) & (place < first + z.distinct)
        out[z.data_rows :, :] = jnp.where(mine, meta, 0)


def first_send(
    z,
    me_ref,
    labels_ref,
    spread_ref,
    owner_ref,
    weight_ref,
    taper_ref,
    real_hbm,
    imag_hbm,
    *refs,
):
    outs = refs[: z.owners]
    slot_out, rank_out, real, imag, sems = refs[z.owners :]
    copy_real = pltpu.make_async_copy(real_hbm, real, sems.at[0])
    copy_imag = pltpu.make_async_copy(imag_hbm, imag, sems.at[1])
    copy_real.start()
    copy_imag.start()
    row_slot, slot_rank = place_groups(z, me_ref[0], labels_ref, spread_ref, owner_ref)
    slot_out[...] = row_slot
    rank_out[...] = slot_rank
    copy_real.wait()
    copy_imag.wait()
    flat = (z.fold, z.channels)
    fold_and_code(
        z,
        0,
        row_slot,
        slot_rank,
        weight_ref,
        taper_ref,
        real[...].reshape(flat),
        imag[...].reshape(flat),
        outs,
    )


def later_send(z, instant, slot_ref, rank_ref, weight_ref, taper_ref, real_ref, imag_ref, *outs):
    flat = (z.fold, z.channels)
    fold_and_code(
        z,
        instant,
        slot_ref[...],
        rank_ref[...],
        weight_ref,
        taper_ref,
        real_ref[...].reshape(flat),
        imag_ref[...].reshape(flat),
        outs,
    )


def spectrum(z, blocks, high_ref, low_ref, twiddle_ref, words):
    meta = blocks[0][z.data_rows :, :]
    for block in blocks[1:]:
        meta = meta + block[z.data_rows :, :]

    def joined(which):
        first = which * z.meta_parts
        return jnp.concatenate([meta[first + p : first + p + 1] for p in range(z.meta_parts)], axis=1)

    rank, weight, code = joined(0), joined(1), joined(2)
    lane = iota((1, z.slot_lanes), 1)
    exponent = code >> 9
    power = jnp.ones((1, z.slot_lanes), F32)
    for bit in range(7):
        power = jnp.where((exponent >> bit) & 1 == 1, power * 2.0 ** (1 << bit), power)
    scale = (code & 511).astype(F32) * power * 2.0 ** -(EXP_BIAS + 22)
    scale = jnp.where(lane % z.stride < z.distinct, scale, 0.0)
    mine = iota((z.per_owner, z.slot_lanes), 0) == rank
    selector = jnp.where(mine, scale, 0.0)[:, : z.slots].astype(BF16)
    total = jnp.sum(jnp.where(mine, weight.astype(F32), 0.0), axis=1, keepdims=True)
    factor = 1.0 / jnp.maximum(total, 1.0)
    for distance, block in enumerate(blocks):
        first = distance * z.stride
        for tile in range(z.tiles):
            words[first : first + z.distinct, tile * LANES : (tile + 1) * LANES] = block[
                pl.ds(tile, z.distinct, stride=z.tiles), :
            ]
        if z.stride > z.distinct:
            words[first + z.distinct : first + z.stride, :] = jnp.zeros(
                (z.stride - z.distinct, z.channels), I32
            )
    word = words[...]

    def mean(coded):
        value = coded.astype(F32) - HALF
        high = value.astype(BF16)
        low = (value - high.astype(F32)).astype(BF16)
        return (dot(selector, high) + dot(selector, low)) * factor

    real = mean(lax.shift_right_logical(word, jnp.full(word.shape, 16, I32)))
    imag = mean(word & 65535)
    quarter = [
        (real[:, m * z.short : (m + 1) * z.short], imag[:, m * z.short : (m + 1) * z.short])
        for m in range(RADIX)
    ]
    even_sum = [a + b for a, b in zip(quarter[0], quarter[2])]
    even_gap = [a - b for a, b in zip(quarter[0], quarter[2])]
    odd_sum = [a + b for a, b in zip(quarter[1], quarter[3])]
    odd_gap = [a - b for a, b in zip(quarter[1], quarter[3])]
    mixed = [
        (even_sum[0] + odd_sum[0], even_sum[1] + odd_sum[1]),
        (even_gap[0] + odd_gap[1], even_gap[1] - odd_gap[0]),
        (even_sum[0] - odd_sum[0], even_sum[1] - odd_sum[1]),
        (even_gap[0] - odd_gap[1], even_gap[1] + odd_gap[0]),
    ]
    turned = [jnp.concatenate(mixed[0], axis=1)]
    for r in range(1, RADIX):
        cosine = twiddle_ref[r : r + 1, :]
        sine = twiddle_ref[RADIX + r : RADIX + r + 1, :]
        a, b = mixed[r]
        turned.append(jnp.concatenate([a * cosine + b * sine, b * cosine - a * sine], axis=1))
    rows = []
    for part in range(z.parts):
        for r in range(RADIX):
            rows.append(turned[r][part * z.share : (part + 1) * z.share])
    data = jnp.concatenate(rows, axis=0)
    high = data.astype(BF16)
    low = (data - high.astype(F32)).astype(BF16)
    table = high_ref[...]
    return dot(high, table) + (dot(low, table) + dot(high, low_ref[...]))


def product(z, a, b):
    wide = a * b
    return wide[:, : z.short] + wide[:, z.short :]


def first_take(z, *refs):
    blocks, (high, low, twiddle, spec_out, words) = refs[: z.owners], refs[z.owners :]
    spec_out[...] = spectrum(z, blocks, high, low, twiddle, words)


def middle_take(z, started, *refs):
    blocks = refs[: z.owners]
    high, low, twiddle, prior, *rest = refs[z.owners :]
    if started:
        running, spec_out, power_out, words = rest
    else:
        spec_out, power_out, words = rest
    spec = spectrum(z, blocks, high, low, twiddle, words)
    power = product(z, prior[...], spec)
    if started:
        power = power + running[...]
    spec_out[...] = spec
    power_out[...] = power


def last_take(z, started, me_ref, *refs):
    blocks = refs[: z.owners]
    high, low, twiddle, prior, following, *rest = refs[z.owners :]
    if started:
        running, *rest = rest
    outs, words, power = rest[: z.parts], rest[z.parts], rest[z.parts + 1]
    spec = spectrum(z, blocks, high, low, twiddle, words)
    total = product(z, spec, prior[...] + following[...])
    if started:
        total = total + running[...]
    power[...] = total
    size = RADIX * z.share
    for distance in range(z.parts):
        start = pl.multiple_of((me_ref[0] ^ distance) * size, SUBLANES)
        outs[distance][...] = power[pl.ds(start, size), :]


def finish(z, *refs):
    parts, out = refs[: z.parts], refs[z.parts]
    total = parts[0][...]
    for part in parts[1:]:
        total = total + part[...]
    width = z.short // RADIX
    rows = []
    for block in range(RADIX):
        rows.append(
            jnp.concatenate(
                [
                    total[r * z.share : (r + 1) * z.share, block * width : (block + 1) * width]
                    for r in range(RADIX)
                ],
                axis=1,
            )
        )
    data = jnp.concatenate(rows, axis=0)
    source = iota((z.short, z.short), 0)
    wanted = source % width * RADIX + source // width
    move = flag(iota((z.short, z.short), 1) == wanted).astype(BF16)
    high = data.astype(BF16)
    rest = data - high.astype(F32)
    middle = rest.astype(BF16)
    low = (rest - middle.astype(F32)).astype(BF16)
    moved = dot(high, move) + (dot(middle, move) + dot(low, move))
    for block in range(RADIX):
        out[:, block * z.short : (block + 1) * z.short] = moved[
            block * z.share : (block + 1) * z.share
        ]


VMEM = pl.BlockSpec(memory_space=pltpu.VMEM)
SMEM = pl.BlockSpec(memory_space=pltpu.SMEM)
ANY = pl.BlockSpec(memory_space=pl.ANY)


def call(body, specs, shapes, scratch, flops, name):
    return pl.pallas_call(
        body,
        in_specs=specs,
        out_specs=jax.tree.map(lambda _: VMEM, shapes),
        out_shape=shapes,
        scratch_shapes=scratch,
        cost_estimate=pl.CostEstimate(flops=flops, bytes_accessed=1 << 20, transcendentals=0),
        name=name,
    )


def swap(block, axis, distance):
    devices = range(lax.axis_size(axis))
    return lax.ppermute(block, axis, [(i, i ^ distance) for i in devices])


def per_device(visibility_real, visibility_imag, weights, labels, owner_of):
    row_count, times, channels = visibility_real.shape
    z = Sizes(
        row_count,
        times,
        channels,
        owner_of.shape[0],
        lax.axis_size("bl"),
        lax.axis_size("tm"),
    )
    me = lax.axis_index("bl").astype(I32).reshape(1)
    my_part = lax.axis_index("tm").astype(I32).reshape(1)
    taper = jnp.asarray(taper_table(channels))
    high, low = (jnp.asarray(table) for table in short_tables(z.short))
    twiddle = jnp.asarray(twiddle_table(channels))
    tables = (high, low, twiddle)
    spread = jnp.broadcast_to(labels[:, None], (row_count, times)).reshape(1, z.fold)
    weight = weights.reshape(1, z.fold)
    block_shape = jax.ShapeDtypeStruct((z.block_rows, LANES), I32)
    sends = [block_shape] * z.owners
    resident = pltpu.VMEM(visibility_real.shape, visibility_real.dtype)
    fold_flops = 4 * z.slots * z.fold * channels
    *blocks, row_slot, slot_rank = call(
        functools.partial(first_send, z),
        [SMEM, VMEM, VMEM, VMEM, VMEM, VMEM, ANY, ANY],
        sends
        + [
            jax.ShapeDtypeStruct((SUBLANES, z.fold), I32),
            jax.ShapeDtypeStruct((SUBLANES, z.slot_lanes), I32),
        ],
        [resident, resident, pltpu.SemaphoreType.DMA((2,))],
        fold_flops,
        "fold_first",
    )(
        me,
        labels.reshape(1, row_count),
        spread,
        owner_of.reshape(1, z.groups),
        weight,
        taper,
        visibility_real,
        visibility_imag,
    )

    def exchange(blocks):
        return [blocks[0]] + [swap(blocks[d], "bl", d) for d in range(1, z.owners)]

    arrived = [exchange(blocks)]
    for instant in range(1, times):
        blocks = call(
            functools.partial(later_send, z, instant),
            [VMEM] * 6,
            sends,
            [],
            fold_flops,
            "fold_later",
        )(row_slot, slot_rank, weight, taper, visibility_real, visibility_imag)
        arrived.append(exchange(blocks))

    spec_shape = jax.ShapeDtypeStruct((RADIX * z.per_owner, 2 * z.short), F32)
    power_shape = jax.ShapeDtypeStruct((RADIX * z.per_owner, z.short), F32)
    part_shape = jax.ShapeDtypeStruct((RADIX * z.share, z.short), F32)
    words = pltpu.VMEM((z.slots, channels), I32)
    take_flops = 3 * 2 * RADIX * z.per_owner * (2 * z.short) ** 2
    base_specs = [VMEM] * (z.owners + 3)
    spec = call(
        functools.partial(first_take, z), base_specs, spec_shape, [words], take_flops, "take_first"
    )(*arrived[0], *tables)
    last = lax.axis_size("tm")
    following = lax.ppermute(spec, "tm", [(i, i - 1) for i in range(1, last)])
    running = ()
    for instant in range(1, times - 1):
        spec, power = call(
            functools.partial(middle_take, z, bool(running)),
            base_specs + [VMEM] * (1 + len(running)),
            [spec_shape, power_shape],
            [words],
            take_flops,
            "take_middle",
        )(*arrived[instant], *tables, spec, *running)
        running = (power,)
    shares = call(
        functools.partial(last_take, z, bool(running)),
        [SMEM] + base_specs + [VMEM] * (2 + len(running)),
        [part_shape] * z.parts,
        [words, pltpu.VMEM(power_shape.shape, F32)],
        take_flops,
        "take_last",
    )(my_part, *arrived[-1], *tables, spec, following, *running)
    gathered = [shares[0]] + [swap(shares[d], "tm", d) for d in range(1, z.parts)]
    return call(
        functools.partial(finish, z),
        [VMEM] * z.parts,
        jax.ShapeDtypeStruct((z.share, channels), F32),
        [],
        1 << 20,
        "finish",
    )(*gathered)


def solution(mesh):
    placed = (P("bl", "tm", None), P("bl", "tm", None), P("bl", "tm"), P("bl"), P())
    return jax.shard_map(
        per_device, mesh=mesh, in_specs=placed, out_specs=P(("bl", "tm"), None), check_vma=False
    )
```

```python
import functools
import math

import jax
import jax.numpy as jnp
import numpy as np
from jax import lax
from jax.experimental import pallas as pl
from jax.experimental.pallas import tpu as pltpu
from jax.sharding import PartitionSpec as P


HARRIS = (0.35875, 0.48829, 0.14128, 0.01168)
LANES = 128
SUBLANES = 8
RADIX = 4
HALF = 32768.0
VMEM_GRANT = 24 << 20
VMEM_WHOLE = 67_043_328
EXP_BIAS = 80
BF16 = jnp.bfloat16
F32 = jnp.float32
I32 = jnp.int32


def up_to(value, multiple):
    return -(-value // multiple) * multiple


class Sizes:
    def __init__(self, rows, times, channels, groups, owners, parts):
        self.rows, self.times, self.channels = rows, times, channels
        self.groups, self.owners, self.parts = groups, owners, parts
        self.per_owner = groups // owners
        capacity = 3 * rows // (2 * owners)
        self.distinct = min(capacity // 4, self.per_owner // 2)
        self.whole = self.distinct // SUBLANES * SUBLANES
        self.rest = self.distinct - self.whole
        self.slots = owners * self.distinct
        self.slot_lanes = up_to(self.slots, LANES)
        self.meta_parts = self.slot_lanes // LANES
        self.tiles = channels // LANES
        self.data_rows = self.distinct * self.tiles
        self.fold = rows * times
        self.short = channels // RADIX
        self.share = self.per_owner // parts

    def meta_rows(self, count, ranked):
        return up_to((2 * count + ranked) * self.meta_parts, SUBLANES)

    def block_rows(self, count, ranked):
        return count * self.data_rows + self.meta_rows(count, ranked)

    def runs(self, distance):
        found = []
        if self.whole:
            found.append((distance * self.whole, 0, self.whole))
        if self.rest:
            found.append((self.owners * self.whole + distance * self.rest, self.whole, self.rest))
        return found


def taper_table(channels):
    angle = 2.0 * math.pi / channels * np.arange(channels, dtype=np.float64)
    window = (
        HARRIS[0]
        - HARRIS[1] * np.cos(angle)
        + HARRIS[2] * np.cos(2.0 * angle)
        - HARRIS[3] * np.cos(3.0 * angle)
    )
    window = window / np.sqrt(np.sum(window * window))
    return window.astype(np.float32)[None, :]


def short_tables(short):
    index = np.arange(short)
    angle = 2.0 * math.pi / short * (index[:, None] * index[None, :] % short)
    cosine, sine = np.cos(angle), np.sin(angle)
    table = np.block([[cosine, -sine], [sine, cosine]]).astype(np.float32)
    high = table.astype(BF16)
    low = (table - high.astype(np.float32)).astype(BF16)
    return high, low


def twiddle_table(channels):
    short = channels // RADIX
    angle = 2.0 * math.pi / channels * (np.arange(RADIX)[:, None] * np.arange(short)[None, :])
    return np.concatenate([np.cos(angle), np.sin(angle)], axis=0).astype(np.float32)


def iota(shape, dimension):
    return lax.broadcasted_iota(I32, shape, dimension)


def dot(a, b):
    return jnp.dot(a, b, preferred_element_type=F32)


def dot_rows(a, b):
    return lax.dot_general(a, b, (((1,), (1,)), ((), ())), preferred_element_type=F32)


def flag(condition):
    return jnp.where(condition, 1.0, 0.0).astype(F32)


def joined(rows):
    return jnp.concatenate([rows[i : i + 1] for i in range(rows.shape[0])], axis=1)


def place_groups(z, me, labels_ref, owner_ref, weight_ref):
    distance = joined(owner_ref[...]) ^ me
    hits = flag(iota((z.owners, z.groups), 0) == distance)
    match = flag(iota((z.groups, z.rows), 0) == joined(labels_ref[...])).astype(BF16)
    counts = dot_rows(jnp.ones((SUBLANES, z.rows), BF16), match)
    present = flag(counts[:1] > 0.5)
    before = flag(iota((z.groups, z.groups), 0) < iota((z.groups, z.groups), 1)).astype(BF16)
    stacked = jnp.concatenate([hits, hits * present], axis=0).astype(BF16)
    prefix = dot(stacked, before)
    rank = jnp.sum(hits * prefix[: z.owners], axis=0, keepdims=True)
    order = jnp.sum(hits * prefix[z.owners :], axis=0, keepdims=True)
    near = distance.astype(F32)
    slot = jnp.where(
        order < z.whole,
        near * z.whole + order,
        near * z.rest + (order + (z.owners * z.whole - z.whole)),
    )
    wide = jnp.broadcast_to(slot, (SUBLANES, z.groups)).astype(BF16)
    row_slot = dot(wide, match)
    narrow = jnp.concatenate(
        [row_slot, weight_ref[...].astype(F32), jnp.zeros((SUBLANES - z.times, z.rows), F32)],
        axis=0,
    ).astype(BF16)
    widen = flag(iota((z.rows, z.fold), 1) // z.times == iota((z.rows, z.fold), 0)).astype(BF16)
    spread = dot(narrow, widen).astype(I32)
    slot_hit = flag(
        (iota((z.slot_lanes, z.groups), 0) == slot.astype(I32)) & (present > 0.5)
    ).astype(BF16)
    ranks = jnp.broadcast_to(rank, (SUBLANES, z.groups)).astype(BF16)
    slot_rank = dot_rows(ranks, slot_hit).astype(I32)
    return spread, slot_rank


def make_folder(z, instant, spread):
    lane = iota((1, z.fold), 1)
    weight = spread[SUBLANES + instant : SUBLANES + instant + 1].astype(F32)
    weight = jnp.where(lane % z.times == instant, weight, 0.0)
    return jnp.where(iota((z.slots, z.fold), 0) == spread[:1], weight, 0.0).astype(BF16)


def code_sums(z, sum_real, sum_imag):
    top = jnp.max(jnp.maximum(jnp.abs(sum_real), jnp.abs(sum_imag)), axis=1, keepdims=True)
    mantissa = jnp.maximum(top, 2.0**-EXP_BIAS) * 2.0**EXP_BIAS
    exponent = jnp.zeros_like(top)
    shrink = jnp.ones_like(top)
    for step in (64, 32, 16, 8, 4, 2, 1):
        large = mantissa >= 2.0**step
        mantissa = jnp.where(large, mantissa * 2.0**-step, mantissa)
        exponent = jnp.where(large, exponent + step, exponent)
        shrink = jnp.where(large, shrink * 2.0**-step, shrink)
    digits = jnp.ceil(mantissa * 128.0)
    inverse = (shrink * 2.0**EXP_BIAS) * (2.0**22 / digits)
    code = exponent * 512.0 + digits
    diagonal = iota((z.slots, z.slot_lanes), 0) == iota((z.slots, z.slot_lanes), 1)
    code_row = jnp.sum(jnp.where(diagonal, code, 0.0), axis=0, keepdims=True).astype(I32)
    top_code = 2.0 * HALF - 1.0
    word_real = jnp.minimum(sum_real * inverse + (HALF + 0.5), top_code).astype(I32)
    word_imag = jnp.minimum(sum_imag * inverse + (HALF + 0.5), top_code).astype(I32)
    return (word_real << 16) | word_imag, code_row


def fold_and_code(z, instants, spread, slot_rank, taper_ref, real, imag, outs):
    count = len(instants)
    folders = [make_folder(z, instant, spread) for instant in instants]
    folder = folders[0] if count == 1 else jnp.concatenate(folders, axis=0)
    taper = taper_ref[...]
    sum_real = dot(folder, real) * taper
    sum_imag = dot(folder, imag) * taper
    rows = [] if slot_rank is None else [slot_rank]
    codes = []
    for at in range(count):
        padded = folders[at]
        if z.slot_lanes > z.slots:
            padded = jnp.concatenate(
                [padded, jnp.zeros((z.slot_lanes - z.slots, z.fold), BF16)], axis=0
            )
        rows.append(dot_rows(jnp.ones((SUBLANES, z.fold), BF16), padded).astype(I32))
        mine = slice(at * z.slots, (at + 1) * z.slots)
        word, code_row = code_sums(z, sum_real[mine], sum_imag[mine])
        codes.append(code_row)
        for distance in range(z.owners):
            for slot, place, size in z.runs(distance):
                start = at * z.data_rows + place * z.tiles
                for tile in range(z.tiles):
                    outs[distance][pl.ds(start + tile, size, stride=z.tiles), :] = word[
                        slot : slot + size, tile * LANES : (tile + 1) * LANES
                    ]
    lines = []
    for row in rows + codes:
        for part in range(z.meta_parts):
            lines.append(row[:1, part * LANES : (part + 1) * LANES])
    meta_rows = z.meta_rows(count, slot_rank is not None)
    if meta_rows > len(lines):
        lines.append(jnp.zeros((meta_rows - len(lines), LANES), I32))
    meta = jnp.concatenate(lines, axis=0)
    lane = iota(meta.shape, 0) % z.meta_parts * LANES + iota(meta.shape, 1)
    for distance in range(z.owners):
        mine = lane < 0
        for slot, _, size in z.runs(distance):
            mine = mine | ((lane >= slot) & (lane < slot + size))
        outs[distance][count * z.data_rows :, :] = jnp.where(mine, meta, 0)


def send(z, instants, count, *refs):
    first = instants[0] == 0
    if first:
        me_ref, *refs = refs
    sources, outs, refs = refs[:count], refs[count : count + z.owners], refs[count + z.owners :]
    if first:
        spread_out, *refs = refs
    targets, sems = refs[:count], refs[count]
    copies = [
        pltpu.make_async_copy(source, target, sems.at[i])
        for i, (source, target) in enumerate(zip(sources, targets))
    ]
    for copy in copies:
        copy.start()
    for copy in copies[:-2]:
        copy.wait()
    *small, taper_ref, real, imag = targets
    if first:
        spread, slot_rank = place_groups(z, me_ref[0], *small)
        spread_out[...] = spread
    else:
        spread, slot_rank = small[0][...], None
    for copy in copies[-2:]:
        copy.wait()
    flat = (z.fold, z.channels)
    fold_and_code(
        z,
        instants,
        spread,
        slot_rank,
        taper_ref,
        real[...].reshape(flat),
        imag[...].reshape(flat),
        outs,
    )


def sum_meta(z, blocks, count):
    meta = blocks[0][count * z.data_rows :, :]
    for block in blocks[1:]:
        meta = meta + block[count * z.data_rows :, :]
    return meta


def meta_line(z, meta, which):
    return joined(meta[which * z.meta_parts : (which + 1) * z.meta_parts])


def means(z, at, blocks, rank, weight, code, words):
    lanes = (1, z.slot_lanes)
    exponent = code >> 9
    power = jnp.ones(lanes, F32)
    for bit in range(7):
        power = jnp.where((exponent >> bit) & 1 == 1, power * 2.0 ** (1 << bit), power)
    scale = (code & 511).astype(F32) * power * 2.0 ** -(EXP_BIAS + 22)
    mine = iota((z.per_owner, z.slot_lanes), 0) == rank
    selector = jnp.where(mine, scale, 0.0)[:, : z.slots].astype(BF16)
    total = jnp.sum(jnp.where(mine, weight.astype(F32), 0.0), axis=1, keepdims=True)
    factor = 1.0 / jnp.maximum(total, 1.0)
    for distance, block in enumerate(blocks):
        for slot, place, size in z.runs(distance):
            start = at * z.data_rows + place * z.tiles
            for tile in range(z.tiles):
                words[slot : slot + size, tile * LANES : (tile + 1) * LANES] = block[
                    pl.ds(start + tile, size, stride=z.tiles), :
                ]
    word = words[...]

    def mean(coded):
        value = coded.astype(F32) - HALF
        high = value.astype(BF16)
        low = (value - high.astype(F32)).astype(BF16)
        return (dot(selector, high) + dot(selector, low)) * factor

    real = mean(lax.shift_right_logical(word, jnp.full(word.shape, 16, I32)))
    imag = mean(word & 65535)
    return real, imag


def residues(z, real, imag, twiddle_ref):
    quarter = [
        (real[:, m * z.short : (m + 1) * z.short], imag[:, m * z.short : (m + 1) * z.short])
        for m in range(RADIX)
    ]
    even_sum = [a + b for a, b in zip(quarter[0], quarter[2])]
    even_gap = [a - b for a, b in zip(quarter[0], quarter[2])]
    odd_sum = [a + b for a, b in zip(quarter[1], quarter[3])]
    odd_gap = [a - b for a, b in zip(quarter[1], quarter[3])]
    mixed = [
        (even_sum[0] + odd_sum[0], even_sum[1] + odd_sum[1]),
        (even_gap[0] + odd_gap[1], even_gap[1] - odd_gap[0]),
        (even_sum[0] - odd_sum[0], even_sum[1] - odd_sum[1]),
        (even_gap[0] - odd_gap[1], even_gap[1] + odd_gap[0]),
    ]
    turned = [jnp.concatenate(mixed[0], axis=1)]
    for r in range(1, RADIX):
        cosine = twiddle_ref[r : r + 1, :]
        sine = twiddle_ref[RADIX + r : RADIX + r + 1, :]
        a, b = mixed[r]
        turned.append(jnp.concatenate([a * cosine + b * sine, b * cosine - a * sine], axis=1))
    rows = []
    for part in range(z.parts):
        for r in range(RADIX):
            rows.append(turned[r][part * z.share : (part + 1) * z.share])
    return jnp.concatenate(rows, axis=0)


def transform(data, high_ref, low_ref):
    high = data.astype(BF16)
    low = (data - high.astype(F32)).astype(BF16)
    table = high_ref[...]
    return dot(high, table) + (dot(low, table) + dot(high, low_ref[...]))


def product(z, a, b):
    wide = a * b
    return wide[:, : z.short] + wide[:, z.short :]


def take(z, kind, count, names, *refs):
    held, (*outs, words) = dict(zip(names, refs[: len(names)])), refs[len(names) :]
    blocks = [held[f"block{d}"] for d in range(z.owners)]
    meta = sum_meta(z, blocks, count)
    first = kind == "first"
    rank = meta_line(z, meta if first else held["ranks"][...], 0)
    spectra = []
    for at in range(count):
        weight = meta_line(z, meta, first + at)
        code = meta_line(z, meta, first + count + at)
        real, imag = means(z, at, blocks, rank, weight, code, words)
        data = residues(z, real, imag, held["twiddle"])
        spectra.append(transform(data, held["high"], held["low"]))
    if first:
        outs[0][...] = spectra[0]
        outs[1][...] = meta
        return
    total = product(z, held["prior"][...], spectra[0])
    for earlier, later in zip(spectra[:-1], spectra[1:]):
        total = total + product(z, earlier, later)
    if "running" in names:
        total = total + held["running"][...]
    if kind == "middle":
        outs[0][...] = spectra[-1]
        outs[1][...] = total
        return
    outs[0][...] = total + product(z, spectra[-1], held["following"][...])


def finish(z, parts, out):
    size = RADIX * z.share
    total = parts[:size]
    for part in range(1, z.parts):
        total = total + parts[part * size : (part + 1) * size]
    width = z.short // RADIX
    rows = []
    for block in range(RADIX):
        rows.append(
            jnp.concatenate(
                [
                    total[r * z.share : (r + 1) * z.share, block * width : (block + 1) * width]
                    for r in range(RADIX)
                ],
                axis=1,
            )
        )
    data = jnp.concatenate(rows, axis=0)
    source = iota((z.short, z.short), 0)
    wanted = source % width * RADIX + source // width
    move = flag(iota((z.short, z.short), 1) == wanted).astype(BF16)
    high = data.astype(BF16)
    rest = data - high.astype(F32)
    middle = rest.astype(BF16)
    low = (rest - middle.astype(F32)).astype(BF16)
    moved = dot(high, move) + (dot(middle, move) + dot(low, move))
    for block in range(RADIX):
        out[:, block * z.short : (block + 1) * z.short] = moved[
            block * z.share : (block + 1) * z.share
        ]


VMEM = pl.BlockSpec(memory_space=pltpu.VMEM)
SMEM = pl.BlockSpec(memory_space=pltpu.SMEM)
HBM = pl.BlockSpec(memory_space=pltpu.HBM)


def call(body, specs, shapes, scratch, flops, grant=VMEM_GRANT):
    return pl.pallas_call(
        body,
        in_specs=specs,
        out_specs=jax.tree.map(lambda _: VMEM, shapes),
        out_shape=shapes,
        scratch_shapes=scratch,
        compiler_params=pltpu.CompilerParams(vmem_limit_bytes=grant),
        cost_estimate=pl.CostEstimate(flops=flops, bytes_accessed=1 << 20, transcendentals=0),
    )


def swap(block, axis, distance):
    devices = range(lax.axis_size(axis))
    return lax.ppermute(block, axis, [(i, i ^ distance) for i in devices])


def far_first(count):
    return [*range(count // 2, count), *range(1, count // 2)]


def per_device(visibility_real, visibility_imag, weights, labels, owner_of):
    row_count, times, channels = visibility_real.shape
    z = Sizes(
        row_count,
        times,
        channels,
        owner_of.shape[0],
        lax.axis_size("bl"),
        lax.axis_size("tm"),
    )
    me = lax.axis_index("bl").astype(I32).reshape(1)
    taper = jnp.asarray(taper_table(channels))
    high, low = (jnp.asarray(table) for table in short_tables(z.short))
    twiddle = jnp.asarray(twiddle_table(channels))
    fold_flops = 4 * z.slots * z.fold * channels
    chunks = [(0,), tuple(range(1, times - 1)), (times - 1,)]
    chunks = [chunk for chunk in chunks if chunk]

    def sends(chunk):
        rows = z.block_rows(len(chunk), chunk[0] == 0)
        return [jax.ShapeDtypeStruct((rows, LANES), I32)] * z.owners

    def exchange(blocks):
        moved = {}
        for d in far_first(z.owners):
            moved[d] = swap(blocks[d], "bl", d)
        return [blocks[0]] + [moved[d] for d in range(1, z.owners)]

    def fold(at, inputs, extra_outs):
        chunk = chunks[at]
        return call(
            functools.partial(send, z, chunk, len(inputs)),
            [SMEM] * (at == 0) + [HBM] * len(inputs),
            sends(chunk) + extra_outs,
            [pltpu.VMEM(value.shape, value.dtype) for value in inputs]
            + [pltpu.SemaphoreType.DMA((len(inputs),))],
            fold_flops * len(chunk),
            grant=VMEM_WHOLE,
        )(*([me] * (at == 0)), *inputs)

    large = (taper, visibility_real, visibility_imag)
    places = (
        labels.reshape(row_count // LANES, LANES),
        owner_of.reshape(z.groups // LANES, LANES),
        weights.T,
    )
    spread_shape = jax.ShapeDtypeStruct((2 * SUBLANES, z.fold), I32)
    *blocks, spread = fold(0, places + large, [spread_shape])
    arrived = [exchange(blocks)]
    for at in range(1, len(chunks)):
        arrived.append(exchange(fold(at, (spread,) + large, [])))

    spec_shape = jax.ShapeDtypeStruct((RADIX * z.per_owner, 2 * z.short), F32)
    power_shape = jax.ShapeDtypeStruct((RADIX * z.per_owner, z.short), F32)
    take_flops = 3 * 2 * RADIX * z.per_owner * (2 * z.short) ** 2
    state = {"twiddle": twiddle, "high": high, "low": low}

    def taken(kind, at, shapes, extra):
        inputs = {f"block{d}": block for d, block in enumerate(arrived[at])} | extra
        names = tuple(inputs)
        values = list(inputs.values())
        scratch = [pltpu.VMEM((z.slots, channels), I32)]
        specs = [VMEM] * len(values)
        count = len(chunks[at])
        body = functools.partial(take, z, kind, count, names)
        return call(body, specs, shapes, scratch, take_flops * count)(*values)

    meta_shape = jax.ShapeDtypeStruct((z.meta_rows(1, True), LANES), I32)
    spec, ranks = taken("first", 0, [spec_shape, meta_shape], state)
    following = lax.ppermute(spec, "tm", [(i, i - 1) for i in range(1, z.parts)])
    running = {}
    if len(chunks) > 2:
        spec, power = taken(
            "middle", 1, [spec_shape, power_shape], state | {"ranks": ranks, "prior": spec}
        )
        running = {"running": power}
    (power,) = taken(
        "last",
        len(chunks) - 1,
        [power_shape],
        {"ranks": ranks} | state | {"prior": spec, "following": following} | running,
    )
    gathered = lax.all_to_all(power, "tm", split_axis=0, concat_axis=0, tiled=True)
    return call(
        functools.partial(finish, z),
        [VMEM],
        jax.ShapeDtypeStruct((z.share, channels), F32),
        [],
        1 << 20,
    )(gathered)


def solution(mesh):
    placed = (P("bl", "tm", None), P("bl", "tm", None), P("bl", "tm"), P("bl"), P())
    return jax.shard_map(
        per_device, mesh=mesh, in_specs=placed, out_specs=P(("bl", "tm"), None), check_vma=False
    )
```

```python
import functools
import math

import jax
import jax.numpy as jnp
import numpy as np
from jax import lax
from jax.experimental import pallas as pl
from jax.experimental.pallas import tpu as pltpu
from jax.sharding import PartitionSpec as P


HARRIS = (0.35875, 0.48829, 0.14128, 0.01168)
LANES = 128
SUBLANES = 8
RADIX = 4
HALF = 32768.0
VMEM_GRANT = 24 << 20
VMEM_WHOLE = 67_043_328
VMEM_MOST = VMEM_WHOLE - (5 << 19)
PIECES = 3
EXP_BIAS = 80
BF16 = jnp.bfloat16
F32 = jnp.float32
I32 = jnp.int32


def up_to(value, multiple):
    return -(-value // multiple) * multiple


class Sizes:
    def __init__(self, rows, times, channels, groups, owners, parts):
        self.rows, self.times, self.channels = rows, times, channels
        self.groups, self.owners, self.parts = groups, owners, parts
        self.per_owner = groups // owners
        capacity = 3 * rows // (2 * owners)
        self.distinct = min(capacity // 4, self.per_owner // 2)
        self.whole = self.distinct // SUBLANES * SUBLANES
        self.rest = self.distinct - self.whole
        self.slots = owners * self.distinct
        self.slot_lanes = up_to(self.slots, LANES)
        self.meta_parts = self.slot_lanes // LANES
        self.tiles = channels // LANES
        self.data_rows = self.distinct * self.tiles
        self.fold = rows * times
        self.short = channels // RADIX
        self.share = self.per_owner // parts

    def meta_rows(self, count, ranked):
        return up_to((2 * count + ranked) * self.meta_parts, SUBLANES)

    def block_rows(self, count, ranked):
        return count * self.data_rows + self.meta_rows(count, ranked)

    def runs(self, distance):
        found = []
        if self.whole:
            found.append((distance * self.whole, 0, self.whole))
        if self.rest:
            found.append((self.owners * self.whole + distance * self.rest, self.whole, self.rest))
        return found


def taper_table(channels):
    angle = 2.0 * math.pi / channels * np.arange(channels, dtype=np.float64)
    window = (
        HARRIS[0]
        - HARRIS[1] * np.cos(angle)
        + HARRIS[2] * np.cos(2.0 * angle)
        - HARRIS[3] * np.cos(3.0 * angle)
    )
    window = window / np.sqrt(np.sum(window * window))
    return window.astype(np.float32)[None, :]


def short_tables(short):
    index = np.arange(short)
    angle = 2.0 * math.pi / short * (index[:, None] * index[None, :] % short)
    cosine, sine = np.cos(angle), np.sin(angle)
    table = np.block([[cosine, -sine], [sine, cosine]]).astype(np.float32)
    high = table.astype(BF16)
    low = (table - high.astype(np.float32)).astype(BF16)
    return high, low


def twiddle_table(channels):
    short = channels // RADIX
    angle = 2.0 * math.pi / channels * (np.arange(RADIX)[:, None] * np.arange(short)[None, :])
    return np.concatenate([np.cos(angle), np.sin(angle)], axis=0).astype(np.float32)


def iota(shape, dimension):
    return lax.broadcasted_iota(I32, shape, dimension)


def dot(a, b):
    return jnp.dot(a, b, preferred_element_type=F32)


def dot_rows(a, b):
    return lax.dot_general(a, b, (((1,), (1,)), ((), ())), preferred_element_type=F32)


def flag(condition):
    return jnp.where(condition, 1.0, 0.0).astype(F32)


def joined(rows):
    return jnp.concatenate([rows[i : i + 1] for i in range(rows.shape[0])], axis=1)


def place_groups(z, me, labels_ref, owner_ref, weight_ref):
    distance = joined(owner_ref[...]) ^ me
    hits = flag(iota((z.owners, z.groups), 0) == distance)
    match = flag(iota((z.groups, z.rows), 0) == joined(labels_ref[...])).astype(BF16)
    counts = dot_rows(jnp.ones((SUBLANES, z.rows), BF16), match)
    present = flag(counts[:1] > 0.5)
    before = flag(iota((z.groups, z.groups), 0) < iota((z.groups, z.groups), 1)).astype(BF16)
    stacked = jnp.concatenate([hits, hits * present], axis=0).astype(BF16)
    prefix = dot(stacked, before)
    rank = jnp.sum(hits * prefix[: z.owners], axis=0, keepdims=True)
    order = jnp.sum(hits * prefix[z.owners :], axis=0, keepdims=True)
    near = distance.astype(F32)
    slot = jnp.where(
        order < z.whole,
        near * z.whole + order,
        near * z.rest + (order + (z.owners * z.whole - z.whole)),
    )
    wide = jnp.broadcast_to(slot, (SUBLANES, z.groups)).astype(BF16)
    row_slot = dot(wide, match)
    narrow = jnp.concatenate(
        [row_slot, weight_ref[...].astype(F32), jnp.zeros((SUBLANES - z.times, z.rows), F32)],
        axis=0,
    ).astype(BF16)
    widen = flag(iota((z.rows, z.fold), 1) // z.times == iota((z.rows, z.fold), 0)).astype(BF16)
    spread = dot(narrow, widen).astype(I32)
    slot_hit = flag(
        (iota((z.slot_lanes, z.groups), 0) == slot.astype(I32)) & (present > 0.5)
    ).astype(BF16)
    ranks = jnp.broadcast_to(rank, (SUBLANES, z.groups)).astype(BF16)
    slot_rank = dot_rows(ranks, slot_hit).astype(I32)
    return spread, slot_rank


def make_folder(z, instant, spread):
    lane = iota((1, z.fold), 1)
    weight = spread[SUBLANES + instant : SUBLANES + instant + 1].astype(F32)
    weight = jnp.where(lane % z.times == instant, weight, 0.0)
    return jnp.where(iota((z.slots, z.fold), 0) == spread[:1], weight, 0.0).astype(BF16)


def code_sums(z, sum_real, sum_imag):
    top = jnp.max(jnp.maximum(jnp.abs(sum_real), jnp.abs(sum_imag)), axis=1, keepdims=True)
    mantissa = jnp.maximum(top, 2.0**-EXP_BIAS) * 2.0**EXP_BIAS
    exponent = jnp.zeros_like(top)
    shrink = jnp.ones_like(top)
    for step in (64, 32, 16, 8, 4, 2, 1):
        large = mantissa >= 2.0**step
        mantissa = jnp.where(large, mantissa * 2.0**-step, mantissa)
        exponent = jnp.where(large, exponent + step, exponent)
        shrink = jnp.where(large, shrink * 2.0**-step, shrink)
    digits = jnp.ceil(mantissa * 128.0)
    inverse = (shrink * 2.0**EXP_BIAS) * (2.0**22 / digits)
    code = exponent * 512.0 + digits
    diagonal = iota((z.slots, z.slot_lanes), 0) == iota((z.slots, z.slot_lanes), 1)
    code_row = jnp.sum(jnp.where(diagonal, code, 0.0), axis=0, keepdims=True).astype(I32)
    top_code = 2.0 * HALF - 1.0
    word_real = jnp.minimum(sum_real * inverse + (HALF + 0.5), top_code).astype(I32)
    word_imag = jnp.minimum(sum_imag * inverse + (HALF + 0.5), top_code).astype(I32)
    return (word_real << 16) | word_imag, code_row


def code_blocks(z, folders, slot_rank, sum_real, sum_imag, outs):
    count = len(folders)
    rows = [] if slot_rank is None else [slot_rank]
    codes = []
    for at in range(count):
        padded = folders[at]
        if z.slot_lanes > z.slots:
            padded = jnp.concatenate(
                [padded, jnp.zeros((z.slot_lanes - z.slots, z.fold), BF16)], axis=0
            )
        rows.append(dot_rows(jnp.ones((SUBLANES, z.fold), BF16), padded).astype(I32))
        mine = slice(at * z.slots, (at + 1) * z.slots)
        word, code_row = code_sums(z, sum_real[mine], sum_imag[mine])
        codes.append(code_row)
        for distance in range(z.owners):
            for slot, place, size in z.runs(distance):
                start = at * z.data_rows + place * z.tiles
                for tile in range(z.tiles):
                    outs[distance][pl.ds(start + tile, size, stride=z.tiles), :] = word[
                        slot : slot + size, tile * LANES : (tile + 1) * LANES
                    ]
    lines = []
    for row in rows + codes:
        for part in range(z.meta_parts):
            lines.append(row[:1, part * LANES : (part + 1) * LANES])
    meta_rows = z.meta_rows(count, slot_rank is not None)
    if meta_rows > len(lines):
        lines.append(jnp.zeros((meta_rows - len(lines), LANES), I32))
    meta = jnp.concatenate(lines, axis=0)
    lane = iota(meta.shape, 0) % z.meta_parts * LANES + iota(meta.shape, 1)
    for distance in range(z.owners):
        mine = lane < 0
        for slot, _, size in z.runs(distance):
            mine = mine | ((lane >= slot) & (lane < slot + size))
        outs[distance][count * z.data_rows :, :] = jnp.where(mine, meta, 0)


def send(z, instants, count, copied, *refs):
    first = instants[0] == 0
    if first:
        me_ref, *refs = refs
    sources, outs, refs = refs[:count], refs[count : count + z.owners], refs[count + z.owners :]
    if first:
        spread_out, *refs = refs
    copies, pieces = [], [slice(0, z.rows)]
    if copied:
        *targets, sems = refs
        pieces = [slice(i * z.rows // PIECES, (i + 1) * z.rows // PIECES) for i in range(PIECES)]
        pairs = list(zip(sources[:-2], targets[:-2]))
        for piece in pieces:
            pairs += [(a.at[piece], b.at[piece]) for a, b in zip(sources[-2:], targets[-2:])]
        copies = [pltpu.make_async_copy(a, b, sems.at[i]) for i, (a, b) in enumerate(pairs)]
        for copy in copies:
            copy.start()
        for copy in copies[: count - 2]:
            copy.wait()
        sources = targets
    *small, taper_ref, real, imag = sources
    if first:
        spread, slot_rank = place_groups(z, me_ref[0], *small)
        spread_out[...] = spread
    else:
        spread, slot_rank = small[0][...], None
    folders = [make_folder(z, instant, spread) for instant in instants]
    folder = folders[0] if len(folders) == 1 else jnp.concatenate(folders, axis=0)
    sum_real = sum_imag = None
    for at, piece in enumerate(pieces):
        for copy in copies[count - 2 + 2 * at : count + 2 * at]:
            copy.wait()
        depth = (piece.stop - piece.start) * z.times
        left = folder[:, piece.start * z.times : piece.stop * z.times]
        part_real = dot(left, real[piece].reshape(depth, z.channels))
        part_imag = dot(left, imag[piece].reshape(depth, z.channels))
        sum_real = part_real if at == 0 else sum_real + part_real
        sum_imag = part_imag if at == 0 else sum_imag + part_imag
    taper = taper_ref[...]
    code_blocks(z, folders, slot_rank, sum_real * taper, sum_imag * taper, outs)


def sum_meta(z, blocks, count):
    meta = blocks[0][count * z.data_rows :, :]
    for block in blocks[1:]:
        meta = meta + block[count * z.data_rows :, :]
    return meta


def meta_line(z, meta, which):
    return joined(meta[which * z.meta_parts : (which + 1) * z.meta_parts])


def means(z, at, blocks, rank, weight, code, words):
    lanes = (1, z.slot_lanes)
    exponent = code >> 9
    power = jnp.ones(lanes, F32)
    for bit in range(7):
        power = jnp.where((exponent >> bit) & 1 == 1, power * 2.0 ** (1 << bit), power)
    scale = (code & 511).astype(F32) * power * 2.0 ** -(EXP_BIAS + 22)
    mine = iota((z.per_owner, z.slot_lanes), 0) == rank
    selector = jnp.where(mine, scale, 0.0)[:, : z.slots].astype(BF16)
    total = jnp.sum(jnp.where(mine, weight.astype(F32), 0.0), axis=1, keepdims=True)
    factor = 1.0 / jnp.maximum(total, 1.0)
    for distance, block in enumerate(blocks):
        for slot, place, size in z.runs(distance):
            start = at * z.data_rows + place * z.tiles
            for tile in range(z.tiles):
                words[slot : slot + size, tile * LANES : (tile + 1) * LANES] = block[
                    pl.ds(start + tile, size, stride=z.tiles), :
                ]
    word = words[...]

    def mean(coded):
        value = coded.astype(F32) - HALF
        high = value.astype(BF16)
        low = (value - high.astype(F32)).astype(BF16)
        return (dot(selector, high) + dot(selector, low)) * factor

    real = mean(lax.shift_right_logical(word, jnp.full(word.shape, 16, I32)))
    imag = mean(word & 65535)
    return real, imag


def residues(z, real, imag, twiddle_ref):
    quarter = [
        (real[:, m * z.short : (m + 1) * z.short], imag[:, m * z.short : (m + 1) * z.short])
        for m in range(RADIX)
    ]
    even_sum = [a + b for a, b in zip(quarter[0], quarter[2])]
    even_gap = [a - b for a, b in zip(quarter[0], quarter[2])]
    odd_sum = [a + b for a, b in zip(quarter[1], quarter[3])]
    odd_gap = [a - b for a, b in zip(quarter[1], quarter[3])]
    mixed = [
        (even_sum[0] + odd_sum[0], even_sum[1] + odd_sum[1]),
        (even_gap[0] + odd_gap[1], even_gap[1] - odd_gap[0]),
        (even_sum[0] - odd_sum[0], even_sum[1] - odd_sum[1]),
        (even_gap[0] - odd_gap[1], even_gap[1] + odd_gap[0]),
    ]
    turned = [jnp.concatenate(mixed[0], axis=1)]
    for r in range(1, RADIX):
        cosine = twiddle_ref[r : r + 1, :]
        sine = twiddle_ref[RADIX + r : RADIX + r + 1, :]
        a, b = mixed[r]
        turned.append(jnp.concatenate([a * cosine + b * sine, b * cosine - a * sine], axis=1))
    rows = []
    for part in range(z.parts):
        for r in range(RADIX):
            rows.append(turned[r][part * z.share : (part + 1) * z.share])
    return jnp.concatenate(rows, axis=0)


def transform(data, high_ref, low_ref):
    high = data.astype(BF16)
    low = (data - high.astype(F32)).astype(BF16)
    table = high_ref[...]
    return dot(high, table) + (dot(low, table) + dot(high, low_ref[...]))


def product(z, a, b):
    wide = a * b
    return wide[:, : z.short] + wide[:, z.short :]


def take(z, kind, count, names, *refs):
    refs = list(refs)
    me_ref = refs.pop(0) if kind == "last" else None
    held, refs = dict(zip(names, refs[: len(names)])), refs[len(names) :]
    power = refs.pop() if kind == "last" else None
    *outs, words = refs
    blocks = [held[f"block{d}"] for d in range(z.owners)]
    meta = sum_meta(z, blocks, count)
    first = kind == "first"
    rank = meta_line(z, meta if first else held["ranks"][...], 0)
    spectra = []
    for at in range(count):
        weight = meta_line(z, meta, first + at)
        code = meta_line(z, meta, first + count + at)
        real, imag = means(z, at, blocks, rank, weight, code, words)
        data = residues(z, real, imag, held["twiddle"])
        spectra.append(transform(data, held["high"], held["low"]))
    if first:
        outs[0][...] = spectra[0]
        outs[1][...] = meta
        return
    total = product(z, held["prior"][...], spectra[0])
    for earlier, later in zip(spectra[:-1], spectra[1:]):
        total = total + product(z, earlier, later)
    if "running" in names:
        total = total + held["running"][...]
    if kind == "middle":
        outs[0][...] = spectra[-1]
        outs[1][...] = total
        return
    power[...] = total + product(z, spectra[-1], held["following"][...])
    size = RADIX * z.share
    for distance in range(z.parts):
        start = pl.multiple_of((me_ref[0] ^ distance) * size, SUBLANES)
        outs[distance][...] = power[pl.ds(start, size), :]


def finish(z, *refs):
    *parts, out = refs
    total = parts[0][...]
    for part in parts[1:]:
        total = total + part[...]
    width = z.short // RADIX
    rows = []
    for block in range(RADIX):
        rows.append(
            jnp.concatenate(
                [
                    total[r * z.share : (r + 1) * z.share, block * width : (block + 1) * width]
                    for r in range(RADIX)
                ],
                axis=1,
            )
        )
    data = jnp.concatenate(rows, axis=0)
    source = iota((z.short, z.short), 0)
    wanted = source % width * RADIX + source // width
    move = flag(iota((z.short, z.short), 1) == wanted).astype(BF16)
    high = data.astype(BF16)
    rest = data - high.astype(F32)
    middle = rest.astype(BF16)
    low = (rest - middle.astype(F32)).astype(BF16)
    moved = dot(high, move) + (dot(middle, move) + dot(low, move))
    for block in range(RADIX):
        out[:, block * z.short : (block + 1) * z.short] = moved[
            block * z.share : (block + 1) * z.share
        ]


VMEM = pl.BlockSpec(memory_space=pltpu.VMEM)
SMEM = pl.BlockSpec(memory_space=pltpu.SMEM)
HBM = pl.BlockSpec(memory_space=pltpu.HBM)


def call(body, specs, shapes, scratch, flops, grant=VMEM_GRANT):
    return pl.pallas_call(
        body,
        in_specs=specs,
        out_specs=jax.tree.map(lambda _: VMEM, shapes),
        out_shape=shapes,
        scratch_shapes=scratch,
        compiler_params=pltpu.CompilerParams(vmem_limit_bytes=grant),
        cost_estimate=pl.CostEstimate(flops=flops, bytes_accessed=1 << 20, transcendentals=0),
    )


def swap(block, axis, distance):
    devices = range(lax.axis_size(axis))
    return lax.ppermute(block, axis, [(i, i ^ distance) for i in devices])


def far_first(count):
    return [*range(count // 2, count), *range(1, count // 2)]


def per_device(visibility_real, visibility_imag, weights, labels, owner_of):
    row_count, times, channels = visibility_real.shape
    z = Sizes(
        row_count,
        times,
        channels,
        owner_of.shape[0],
        lax.axis_size("bl"),
        lax.axis_size("tm"),
    )
    me = lax.axis_index("bl").astype(I32).reshape(1)
    my_part = lax.axis_index("tm").astype(I32).reshape(1)
    taper = jnp.asarray(taper_table(channels))
    high, low = (jnp.asarray(table) for table in short_tables(z.short))
    twiddle = jnp.asarray(twiddle_table(channels))
    fold_flops = 4 * z.slots * z.fold * channels
    chunks = [(0,), tuple(range(1, times - 1)), (times - 1,)]
    chunks = [chunk for chunk in chunks if chunk]

    def sends(chunk):
        rows = z.block_rows(len(chunk), chunk[0] == 0)
        return [jax.ShapeDtypeStruct((rows, LANES), I32)] * z.owners

    def exchange(blocks):
        moved = {}
        for d in far_first(z.owners):
            moved[d] = swap(blocks[d], "bl", d)
        return [blocks[0]] + [moved[d] for d in range(1, z.owners)]

    def fold(at, inputs, extra_outs):
        chunk = chunks[at]
        copied = True
        scratch = []
        if copied:
            scratch = [pltpu.VMEM(value.shape, value.dtype) for value in inputs]
            scratch.append(pltpu.SemaphoreType.DMA((len(inputs) - 2 + 2 * PIECES,)))
        return call(
            functools.partial(send, z, chunk, len(inputs), copied),
            [SMEM] * (at == 0) + [HBM if copied else VMEM] * len(inputs),
            sends(chunk) + extra_outs,
            scratch,
            fold_flops * len(chunk),
            grant=VMEM_MOST if at else VMEM_WHOLE,
        )(*([me] * (at == 0)), *inputs)

    large = (taper, visibility_real, visibility_imag)
    places = (
        labels.reshape(row_count // LANES, LANES),
        owner_of.reshape(z.groups // LANES, LANES),
        weights.T,
    )
    spread_shape = jax.ShapeDtypeStruct((2 * SUBLANES, z.fold), I32)
    *blocks, spread = fold(0, places + large, [spread_shape])
    arrived = [exchange(blocks)]
    for at in range(1, len(chunks)):
        arrived.append(exchange(fold(at, (spread,) + large, [])))

    spec_shape = jax.ShapeDtypeStruct((RADIX * z.per_owner, 2 * z.short), F32)
    part_shape = jax.ShapeDtypeStruct((RADIX * z.share, z.short), F32)
    power_shape = jax.ShapeDtypeStruct((RADIX * z.per_owner, z.short), F32)
    take_flops = 3 * 2 * RADIX * z.per_owner * (2 * z.short) ** 2
    state = {"twiddle": twiddle, "high": high, "low": low}

    def taken(kind, at, shapes, extra):
        inputs = {f"block{d}": block for d, block in enumerate(arrived[at])} | extra
        names = tuple(inputs)
        values = list(inputs.values())
        scratch = [pltpu.VMEM((z.slots, channels), I32)]
        specs = [VMEM] * len(values)
        if kind == "last":
            specs = [SMEM] + specs
            values = [my_part] + values
            scratch.append(pltpu.VMEM(power_shape.shape, F32))
        count = len(chunks[at])
        body = functools.partial(take, z, kind, count, names)
        return call(body, specs, shapes, scratch, take_flops * count)(*values)

    meta_shape = jax.ShapeDtypeStruct((z.meta_rows(1, True), LANES), I32)
    spec, ranks = taken("first", 0, [spec_shape, meta_shape], state)
    following = lax.ppermute(spec, "tm", [(i, i - 1) for i in range(1, z.parts)])
    running = {}
    if len(chunks) > 2:
        spec, power = taken(
            "middle", 1, [spec_shape, power_shape], state | {"ranks": ranks, "prior": spec}
        )
        running = {"running": power}
    shares = taken(
        "last",
        len(chunks) - 1,
        [part_shape] * z.parts,
        {"ranks": ranks} | state | {"prior": spec, "following": following} | running,
    )
    moved = [swap(shares[d], "tm", d) for d in range(1, z.parts)]
    return call(
        functools.partial(finish, z),
        [VMEM] * z.parts,
        jax.ShapeDtypeStruct((z.share, channels), F32),
        [],
        1 << 20,
    )(shares[0], *moved)


def solution(mesh):
    placed = (P("bl", "tm", None), P("bl", "tm", None), P("bl", "tm"), P("bl"), P())
    return jax.shard_map(
        per_device, mesh=mesh, in_specs=placed, out_specs=P(("bl", "tm"), None), check_vma=False
    )
```
